32 devices in a mesh: gx: 2 (over core), gy: 4 (over y, x), gz: 4 (over z).
Axes of the slice: x: 2, y: 2, z: 4, core: 2. Of those that a mesh axis runs over, the one named last changes fastest.
Arguments:
- raw_weight: float32 [128, 27, 128], P(('gx', 'gy')), may hold values from -6 to 6
- inputs: bfloat16 [16, 64, 64, 128], P('gx', 'gy', 'gz'), may hold values from -6 to 6
- cotangent: bfloat16 [16, 64, 64, 128], P('gx', 'gy', 'gz'), may hold values from -0.099609375 to 0.099609375
Outputs:
- input_grad: bfloat16 [16, 64, 64, 128], P('gx', 'gy', 'gz')
- weight_grad: float32 [128, 27, 128], P(('gx', 'gy'))
The draws below stay inside these ranges and needn't reach their ends.
All inputs are finite; a program needn't handle non-finite values.
Results may differ from the reference program's by a relative error of at most 0.0049.
Values may be sent and summed in bfloat16 or wider, within the bound.
A program may use at most 64 MiB of HBM per device.

```python
import math
import jax
import jax.numpy as jnp
from jax import lax

C = 128
KK = 27
NX = 16
NY = 64
NZ = 64


def draw_raw_weight(key, part):
    sub_keys = jax.random.split(key, 4)
    row_scale = jnp.exp(jax.random.uniform(sub_keys[0], (C, 1, 1), jnp.float32, math.log(0.1), 0.0))
    col_scale = jnp.exp(jax.random.uniform(sub_keys[1], (1, 1, C), jnp.float32, math.log(0.1), 0.0))
    col_mean = jax.random.uniform(sub_keys[2], (1, 1, C), jnp.float32, -0.5, 0.5)
    base_draw = jnp.clip(jax.random.normal(sub_keys[3], (C, KK, C), jnp.float32), -4.0, 4.0)
    return jnp.clip((base_draw * row_scale + col_mean) * col_scale, -6.0, 6.0)


def steps_of(rng, shape, cuts, smallest, top_value):
    def one(dim, parts):
        steps = jax.random.uniform(jax.random.fold_in(jax.random.fold_in(rng, 6), dim), (parts,), jnp.float32, smallest / len(cuts), top_value / len(cuts))
        return jnp.repeat(jnp.exp(steps), shape[dim] // parts).reshape((-1,) + (1,) * (len(shape) - dim - 1))

    level = one(*cuts[0])
    for cut in cuts[1:]:
        level = level * one(*cut)
    return level


def normal_values(rng, shape, scale, most, shards=(), dtype=jnp.bfloat16):
    array = jax.random.normal(rng, shape, jnp.float32) * scale
    if len(shards) > 0:
        array = steps_of(rng, shape, shards, -0.22, 0.18) * array
    return jnp.clip(array, min=-most, max=most).astype(dtype)


def setup_inputs(seed: int = 0) -> dict:
    key_of = jax.random.split(jax.random.key(seed), 4)
    raw_weight = draw_raw_weight(jax.random.fold_in(key_of[3], 71), 0)
    inputs = normal_values(key_of[1], (NX, NY, NZ, C), 1.0, 6.0, ((0, 2), (1, 4), (2, 4)))
    cotangent = normal_values(key_of[2], (NX, NY, NZ, C), 0.017, 0.099609375, ((0, 2), (1, 4), (2, 4)))
    return dict(raw_weight=raw_weight, inputs=inputs, cotangent=cotangent)


var_eps = 1e-05
norm_eps = 1e-06
clip_norm = 600.0

def tap_view(padded, tap_a, tap_b, tap_c, extent):
    view = padded[2 - tap_a:2 - tap_a + extent[0], 2 - tap_b:2 - tap_b + extent[1], 2 - tap_c:2 - tap_c + extent[2], :]
    return view.reshape(-1, view.shape[-1])

def reference(raw_weight, inputs, cotangent):
    extent = inputs.shape[:3]
    channels = inputs.shape[3]
    fan_count = raw_weight.shape[0] * raw_weight.shape[1]
    sum_first = lax.optimization_barrier(jnp.sum(raw_weight, axis=(0, 1)))
    sum_second = lax.optimization_barrier(jnp.sum(raw_weight * raw_weight, axis=(0, 1)))
    mean_out = sum_first / fan_count
    var_out = sum_second / fan_count - mean_out * mean_out
    inv_std = lax.rsqrt(var_out + var_eps)
    std_float = (raw_weight - mean_out) * inv_std
    std_half = lax.optimization_barrier(std_float.astype(jnp.bfloat16)).astype(jnp.float32)
    padded = jnp.pad(cotangent.astype(jnp.float32), ((1, 1), (1, 1), (1, 1), (0, 0)))
    flat_in = inputs.astype(jnp.float32).reshape(-1, channels)
    dx_total = jnp.zeros((flat_in.shape[0], channels), jnp.float32)
    pieces = []
    for tap_a in range(3):
        for tap_b in range(3):
            for tap_c in range(3):
                tap_index = tap_a * 9 + tap_b * 3 + tap_c
                view = tap_view(padded, tap_a, tap_b, tap_c, extent)
                dx_total = dx_total + jnp.dot(view, std_half[:, tap_index, :].T, precision=lax.Precision.HIGHEST)
                pieces.append(jnp.dot(flat_in.T, view, precision=lax.Precision.HIGHEST))
    input_grad = dx_total.reshape(extent[0], extent[1], extent[2], channels).astype(jnp.bfloat16)
    filter_grad = jnp.stack(pieces, axis=1)
    mean_grad = lax.optimization_barrier(jnp.sum(filter_grad, axis=(0, 1))) / fan_count
    mean_cross = lax.optimization_barrier(jnp.sum(filter_grad * std_float, axis=(0, 1))) / fan_count
    raw_grad = inv_std * (filter_grad - mean_grad - std_float * mean_cross)
    square_sum = jnp.sum(raw_grad * raw_grad)
    scale = jnp.minimum(1.0, clip_norm * lax.rsqrt(square_sum + norm_eps))
    return (input_grad, raw_grad * scale)
```

```python
import functools

import jax
import jax.numpy as jnp
from jax import lax
from jax.experimental import pallas as pl
from jax.experimental.pallas import tpu as pltpu
from jax.sharding import PartitionSpec as P

var_eps = 1e-05
norm_eps = 1e-06
clip_norm = 600.0
F32 = jnp.float32
BF16 = jnp.bfloat16
MESH = pl.DeviceIdType.MESH
AXES = ("gx", "gy", "gz")


def kernel(dims, raw_ref, in_ref, cot_ref, dx_ref, wg_ref, *scratch):
    (shifted, face_out, face_in, in_t, part, recv_x, send_y, recv_y, send_z, recv_z, full, std,
     std_all, w_cat, stats, stats_in, halo_send, halo_recv, x_send, x_recv, y_send, y_recv,
     z_send, z_recv, g_send, g_recv, ay_send, ay_recv, ax_send, ax_recv, st_send, st_recv) = scratch
    count = dict(zip(AXES, dims))
    nx, ny, nz = dims
    me = {axis: lax.axis_index(axis) for axis in AXES}
    rows, taps, chan = raw_ref.shape
    ex, ey, ez = in_ref.shape[:3]
    piece = part.shape[2] // nz
    fan_count = float(rows * nx * ny * taps)

    def peer(axis, k):
        return lax.rem(me[axis] + k, count[axis])

    def remote(src, dst, send_sem, recv_sem, axis, where):
        return pltpu.make_async_remote_copy(
            src_ref=src, dst_ref=dst, send_sem=send_sem, recv_sem=recv_sem,
            device_id={axis: where}, device_id_type=MESH,
        )

    def wait_all(copies):
        for copy in copies:
            copy.wait()

    barrier = pltpu.get_barrier_semaphore()
    for axis in AXES:
        for k in range(1, count[axis]):
            pl.semaphore_signal(barrier, inc=1, device_id={axis: peer(axis, k)}, device_id_type=MESH)

    def exchange_start(slot, axis):
        base = (slot * 2 + (0 if axis == "gx" else 1)) * (max(dims) - 1)
        copies = []
        for k in range(1, count[axis]):
            copy = remote(stats.at[slot * 2 + (0 if axis == "gx" else 1)], stats_in.at[base + k - 1],
                          st_send.at[base + k - 1], st_recv.at[base + k - 1], axis, peer(axis, k))
            copy.start()
            copies.append(copy)
        return copies

    def exchange_sum(slot, axis):
        index = slot * 2 + (0 if axis == "gx" else 1)
        base = index * (max(dims) - 1)
        total = stats[index]
        for k in range(1, count[axis]):
            total = total + stats_in[base + k - 1]
        return total

    raw = raw_ref[...]
    first = jnp.sum(jnp.sum(raw, axis=0), axis=0, keepdims=True)
    second = jnp.sum(jnp.sum(raw * raw, axis=0), axis=0, keepdims=True)
    pad = jnp.zeros((6, chan), F32)
    stats[0] = jnp.concatenate([first, second, pad], axis=0)

    zero_plane = jnp.zeros((ey, ez, chan), BF16)
    zero_col = jnp.zeros((ex + 2, ez, chan), BF16)
    zero_face = jnp.zeros((ex + 2, ey + 2, chan), BF16)

    @pl.when(me["gx"] == 0)
    def _():
        shifted[1, 0, 1:ey + 1] = zero_plane

    @pl.when(me["gx"] == nx - 1)
    def _():
        shifted[1, ex + 1, 1:ey + 1] = zero_plane

    @pl.when(me["gy"] == 0)
    def _():
        shifted[1, :, 0] = zero_col

    @pl.when(me["gy"] == ny - 1)
    def _():
        shifted[1, :, ey + 1] = zero_col

    @pl.when(me["gz"] == 0)
    def _():
        face_in[0] = zero_face

    @pl.when(me["gz"] == nz - 1)
    def _():
        face_in[1] = zero_face

    pl.semaphore_wait(barrier, sum(n - 1 for n in dims))

    def halo(axis, number, low_src, high_dst, high_src, low_dst):
        lower, upper = lax.max(me[axis] - 1, 0), lax.min(me[axis] + 1, count[axis] - 1)
        down = remote(low_src, high_dst, halo_send.at[2 * number], halo_recv.at[2 * number], axis, lower)
        up = remote(high_src, low_dst, halo_send.at[2 * number + 1], halo_recv.at[2 * number + 1], axis, upper)

        @pl.when(me[axis] > 0)
        def _():
            down.start()

        @pl.when(me[axis] < count[axis] - 1)
        def _():
            up.start()

        def finish():
            @pl.when(me[axis] > 0)
            def _():
                down.wait_send()
                up.wait_recv()

            @pl.when(me[axis] < count[axis] - 1)
            def _():
                up.wait_send()
                down.wait_recv()

        return finish

    body = pl.ds(1, ey)
    halo_x = halo("gx", 0, cot_ref.at[0], shifted.at[1, ex + 1, body],
                  cot_ref.at[ex - 1], shifted.at[1, 0, body])
    stats_x = exchange_start(0, "gx")
    shifted[1, 1:ex + 1, 1:ey + 1] = cot_ref[...]
    halo_x()
    halo_y = halo("gy", 1, shifted.at[1, :, 1], shifted.at[1, :, ey + 1],
                  shifted.at[1, :, ey], shifted.at[1, :, 0])
    wait_all(stats_x)
    stats[1] = exchange_sum(0, "gx")
    stats_y = exchange_start(0, "gy")
    for x in range(ex):
        in_t[:, x * ey * ez:(x + 1) * ey * ez] = in_ref[x].reshape(ey * ez, chan).T
    halo_y()
    for x in range(ex + 2):
        plane = shifted[1, x].astype(F32)
        face_out[0, x] = plane[:, 0, :].astype(BF16)
        face_out[1, x] = plane[:, ez - 1, :].astype(BF16)
    halo_z = halo("gz", 2, face_out.at[0], face_in.at[1], face_out.at[1], face_in.at[0])

    wait_all(stats_y)
    sums = exchange_sum(0, "gy")
    mean_out = sums[0:1] / fan_count
    var_out = sums[1:2] / fan_count - mean_out * mean_out
    inv_std = lax.rsqrt(var_out + var_eps)
    own = std_all.at[me["gx"], me["gy"]]
    for t in range(taps):
        value = (raw_ref[:, t, :] - mean_out) * inv_std
        std[t] = value
        own[t] = value.astype(BF16)
    gather_y = []
    for k in range(1, ny):
        copy = remote(own, own, ay_send.at[k - 1], ay_recv.at[k - 1], "gy", peer("gy", k))
        copy.start()
        gather_y.append(copy)

    halo_z()
    depth_index = lax.broadcasted_iota(jnp.int32, (ey + 2, ez, chan), 1)
    for x in range(ex + 2):
        plane = shifted[1, x].astype(F32)
        low = face_in[0, x].astype(F32)[:, None, :]
        high = face_in[1, x].astype(F32)[:, None, :]
        shifted[0, x] = jnp.where(depth_index == 0, low, pltpu.roll(plane, 1, 1)).astype(BF16)
        shifted[2, x] = jnp.where(depth_index == ez - 1, high, pltpu.roll(plane, ez - 1, 1)).astype(BF16)

    def view(t, start, planes):
        a, b, c = t // 9, (t // 3) % 3, t % 3
        block = shifted[2 - c, pl.ds(start + 2 - a, planes), 2 - b:2 - b + ey]
        return block.reshape(planes * ey * ez, chan)

    for t in range(0, taps, 2):
        group = list(range(t, min(t + 2, taps)))
        right = jnp.concatenate([view(s, 0, ex) for s in group], axis=1) if len(group) > 1 else view(t, 0, ex)
        product = jnp.dot(in_t[...], right, preferred_element_type=F32)
        for j, s in enumerate(group):
            for gx in range(nx):
                for gy in range(ny):
                    low = (gx * ny + gy) * rows
                    part[gx, gy, s] = product[low:low + rows, j * chan:(j + 1) * chan]
    for t in range(taps, piece * nz):
        for gx in range(nx):
            for gy in range(ny):
                part[gx, gy, t] = jnp.zeros((rows, chan), F32)
    reduce_x = []
    for k in range(1, nx):
        copy = remote(part.at[peer("gx", k)], recv_x.at[k - 1], x_send.at[k - 1], x_recv.at[k - 1], "gx", peer("gx", k))
        copy.start()
        reduce_x.append(copy)

    wait_all(gather_y)
    gather_x = []
    for k in range(1, nx):
        copy = remote(std_all.at[me["gx"]], std_all.at[me["gx"]], ax_send.at[k - 1], ax_recv.at[k - 1], "gx", peer("gx", k))
        copy.start()
        gather_x.append(copy)

    wait_all(reduce_x)
    for gy in range(ny):
        total = part[me["gx"], gy]
        for k in range(1, nx):
            total = total + recv_x[k - 1, gy]
        send_y[gy] = total.astype(BF16)
    reduce_y = []
    for k in range(1, ny):
        copy = remote(send_y.at[peer("gy", k)], recv_y.at[k - 1], y_send.at[k - 1], y_recv.at[k - 1], "gy", peer("gy", k))
        copy.start()
        reduce_y.append(copy)

    wait_all(gather_x)
    for t in range(taps):
        w_cat[:, t * chan:(t + 1) * chan] = std_all[:, :, t].reshape(nx * ny * rows, chan)
    step = 2 if ex % 2 == 0 else 1

    def dx_step(n, carry):
        start = n * step
        left = jnp.concatenate([view(t, start, step) for t in range(taps)], axis=1)
        product = lax.dot_general(left, w_cat[...], (((1,), (1,)), ((), ())), preferred_element_type=F32)
        dx_ref[pl.ds(start, step)] = product.astype(BF16).reshape(step, ey, ez, chan)
        return carry

    half = ex // step // 2
    lax.fori_loop(0, half, dx_step, 0)

    wait_all(reduce_y)
    total = send_y[me["gy"]].astype(F32)
    for k in range(1, ny):
        total = total + recv_y[k - 1].astype(F32)
    send_z[...] = total.astype(BF16)
    reduce_z = []
    for k in range(1, nz):
        copy = remote(send_z.at[pl.ds(peer("gz", k) * piece, piece)], recv_z.at[k - 1], z_send.at[k - 1], z_recv.at[k - 1], "gz", peer("gz", k))
        copy.start()
        reduce_z.append(copy)

    lax.fori_loop(half, ex // step, dx_step, 0)

    wait_all(reduce_z)
    mine = pl.ds(me["gz"] * piece, piece)
    total = send_z[mine].astype(F32)
    for k in range(1, nz):
        total = total + recv_z[k - 1].astype(F32)
    full[mine] = total
    gather_z = []
    for k in range(1, nz):
        copy = remote(full.at[mine], full.at[mine], g_send.at[k - 1], g_recv.at[k - 1], "gz", peer("gz", k))
        copy.start()
        gather_z.append(copy)
    wait_all(gather_z)

    grad = full[0:taps]
    std_value = std[...]

    def per_output(value):
        return jnp.sum(jnp.sum(value, axis=0), axis=0, keepdims=True)

    stats[2] = jnp.concatenate(
        [per_output(grad), per_output(grad * std_value), per_output(grad * grad), jnp.zeros((5, chan), F32)], axis=0
    )
    wait_all(exchange_start(1, "gx"))
    stats[3] = exchange_sum(1, "gx")
    wait_all(exchange_start(1, "gy"))
    sums = exchange_sum(1, "gy")
    sum_grad, sum_cross, sum_square = sums[0:1], sums[1:2], sums[2:3]
    mean_grad = sum_grad / fan_count
    mean_cross = sum_cross / fan_count
    spread = sum_square - 2.0 * mean_grad * sum_grad - 2.0 * mean_cross * sum_cross
    spread = (
        spread
        + fan_count * mean_grad * mean_grad
        + fan_count * mean_cross * mean_cross * var_out / (var_out + var_eps)
    )
    square_sum = jnp.sum(inv_std * inv_std * spread, axis=1, keepdims=True)
    scale = jnp.minimum(1.0, clip_norm * lax.rsqrt(square_sum + norm_eps))
    factor = inv_std * scale
    for t in range(taps):
        wg_ref[:, t, :] = factor * (full[t] - mean_grad - std[t] * mean_cross)


def on_device(dims, raw_weight, inputs, cotangent):
    nx, ny, nz = dims
    rows, taps, chan = raw_weight.shape
    ex, ey, ez = inputs.shape[:3]
    padded_taps = -(-taps // nz) * nz
    piece = padded_taps // nz
    most = max(dims) - 1
    dma = pltpu.SemaphoreType.DMA

    def pair(n):
        return [dma((max(n, 1),)), dma((max(n, 1),))]

    scratch = [
        pltpu.VMEM((3, ex + 2, ey + 2, ez, chan), BF16),
        pltpu.VMEM((2, ex + 2, ey + 2, chan), BF16),
        pltpu.VMEM((2, ex + 2, ey + 2, chan), BF16),
        pltpu.VMEM((chan, ex * ey * ez), BF16),
        pltpu.VMEM((nx, ny, padded_taps, rows, chan), F32),
        pltpu.VMEM((nx - 1, ny, padded_taps, rows, chan), F32),
        pltpu.VMEM((ny, padded_taps, rows, chan), BF16),
        pltpu.VMEM((ny - 1, padded_taps, rows, chan), BF16),
        pltpu.VMEM((padded_taps, rows, chan), BF16),
        pltpu.VMEM((nz - 1, piece, rows, chan), BF16),
        pltpu.VMEM((padded_taps, rows, chan), F32),
        pltpu.VMEM((taps, rows, chan), F32),
        pltpu.VMEM((nx, ny, taps, rows, chan), BF16),
        pltpu.VMEM((chan, taps * chan), BF16),
        pltpu.VMEM((4, 8, chan), F32),
        pltpu.VMEM((4 * most, 8, chan), F32),
        *pair(6), *pair(nx - 1), *pair(ny - 1), *pair(nz - 1), *pair(nz - 1),
        *pair(ny - 1), *pair(nx - 1), *pair(4 * most),
    ]
    vmem = pl.BlockSpec(memory_space=pltpu.VMEM)
    return pl.pallas_call(
        functools.partial(kernel, dims),
        out_shape=(
            jax.ShapeDtypeStruct(cotangent.shape, BF16),
            jax.ShapeDtypeStruct(raw_weight.shape, F32),
        ),
        in_specs=[vmem] * 3,
        out_specs=(vmem, vmem),
        scratch_shapes=scratch,
        compiler_params=pltpu.CompilerParams(
            collective_id=0, has_side_effects=True, vmem_limit_bytes=48 * 1024 * 1024
        ),
    )(raw_weight, inputs, cotangent)


def solution(mesh):
    dims = tuple(mesh.shape[axis] for axis in AXES)
    in_specs = (P(("gx", "gy"), None, None), P("gx", "gy", "gz", None), P("gx", "gy", "gz", None))
    out_specs = (P("gx", "gy", "gz", None), P(("gx", "gy"), None, None))
    return jax.shard_map(
        functools.partial(on_device, dims), mesh=mesh, in_specs=in_specs, out_specs=out_specs, check_vma=False
    )
```

```python
import functools

import jax
import jax.numpy as jnp
from jax import lax
from jax.experimental import pallas as pl
from jax.experimental.pallas import tpu as pltpu
from jax.sharding import PartitionSpec as P

var_eps = 1e-05
norm_eps = 1e-06
clip_norm = 600.0
F32 = jnp.float32
BF16 = jnp.bfloat16
MESH = pl.DeviceIdType.MESH
AXES = ("gx", "gy", "gz")


def kernel(dims, raw_hbm, in_hbm, cot_hbm, dx_ref, wg_ref, *scratch):
    (raw_ref, in_ref, shifted, face_out, face_in, in_t, part, recv_x, send_y, recv_y, send_z, recv_z, full, std,
     std_all, w_cat, stats, stats_in, load_sem, halo_send, halo_recv, x_send, x_recv, y_send, y_recv,
     z_send, z_recv, g_send, g_recv, ay_send, ay_recv, ax_send, ax_recv, st_send, st_recv) = scratch
    count = dict(zip(AXES, dims))
    nx, ny, nz = dims
    plane_peers = nx * ny - 1
    me = {axis: lax.axis_index(axis) for axis in AXES}
    taps, rows, chan = raw_ref.shape
    ex, ey, ez = in_ref.shape[:3]
    padded_taps = send_z.shape[0]
    piece = padded_taps // nz
    fan_count = float(rows * nx * ny * taps)

    def peer(axis, k):
        return lax.rem(me[axis] + k, count[axis])

    def plane_peer(k):
        flat = lax.rem(me["gx"] * ny + me["gy"] + k, nx * ny)
        return {"gx": lax.div(flat, ny), "gy": lax.rem(flat, ny)}

    def remote(src, dst, send_sem, recv_sem, where):
        return pltpu.make_async_remote_copy(
            src_ref=src, dst_ref=dst, send_sem=send_sem, recv_sem=recv_sem,
            device_id=where, device_id_type=MESH,
        )

    def wait_all(copies):
        for copy in copies:
            copy.wait()

    body = pl.ds(1, ey)
    load_raw = pltpu.make_async_copy(raw_hbm, raw_ref, load_sem.at[0])
    load_cot = pltpu.make_async_copy(cot_hbm, shifted.at[1, pl.ds(1, ex), body], load_sem.at[1])
    load_in = pltpu.make_async_copy(in_hbm, in_ref, load_sem.at[2])
    load_raw.start()
    load_cot.start()
    load_in.start()

    barrier = pltpu.get_barrier_semaphore()
    for k in range(1, nx * ny):
        pl.semaphore_signal(barrier, inc=1, device_id=plane_peer(k), device_id_type=MESH)
    for k in range(1, nz):
        pl.semaphore_signal(barrier, inc=1, device_id={"gz": peer("gz", k)}, device_id_type=MESH)

    def exchange_start(slot, base, peers):
        copies = []
        for k, where in enumerate(peers):
            copy = remote(stats.at[slot], stats_in.at[base + k], st_send.at[base + k], st_recv.at[base + k], where)
            copy.start()
            copies.append(copy)
        return copies

    def exchange_sum(slot, base, copies):
        wait_all(copies)
        total = stats[slot]
        for k in range(len(copies)):
            total = total + stats_in[base + k]
        return total

    zero_plane = jnp.zeros((ey, ez, chan), BF16)
    zero_col = jnp.zeros((ex + 2, ez, chan), BF16)
    zero_face = jnp.zeros((ex + 2, ey + 2, chan), BF16)

    @pl.when(me["gx"] == 0)
    def _():
        shifted[1, 0, 1:ey + 1] = zero_plane

    @pl.when(me["gx"] == nx - 1)
    def _():
        shifted[1, ex + 1, 1:ey + 1] = zero_plane

    @pl.when(me["gy"] == 0)
    def _():
        shifted[1, :, 0] = zero_col

    @pl.when(me["gy"] == ny - 1)
    def _():
        shifted[1, :, ey + 1] = zero_col

    @pl.when(me["gz"] == 0)
    def _():
        face_in[0] = zero_face

    @pl.when(me["gz"] == nz - 1)
    def _():
        face_in[1] = zero_face

    for t in range(taps, padded_taps):
        send_z[t] = jnp.zeros((rows, chan), BF16)
        std[t] = jnp.zeros((rows, chan), F32)

    load_raw.wait()

    def per_output(value):
        return jnp.sum(jnp.sum(value, axis=0), axis=0, keepdims=True)

    raw = raw_ref[...]
    stats[0] = jnp.concatenate([per_output(raw), per_output(raw * raw), jnp.zeros((6, chan), F32)], axis=0)
    load_cot.wait()
    pl.semaphore_wait(barrier, plane_peers + nz - 1)

    def halo(axis, number, low_src, high_dst, high_src, low_dst):
        lower, upper = lax.max(me[axis] - 1, 0), lax.min(me[axis] + 1, count[axis] - 1)
        down = remote(low_src, high_dst, halo_send.at[2 * number], halo_recv.at[2 * number], {axis: lower})
        up = remote(high_src, low_dst, halo_send.at[2 * number + 1], halo_recv.at[2 * number + 1], {axis: upper})

        @pl.when(me[axis] > 0)
        def _():
            down.start()

        @pl.when(me[axis] < count[axis] - 1)
        def _():
            up.start()

        def finish():
            @pl.when(me[axis] > 0)
            def _():
                down.wait_send()
                up.wait_recv()

            @pl.when(me[axis] < count[axis] - 1)
            def _():
                up.wait_send()
                down.wait_recv()

        return finish

    halo_x = halo("gx", 0, shifted.at[1, 1, body], shifted.at[1, ex + 1, body],
                  shifted.at[1, ex, body], shifted.at[1, 0, body])
    weight_sums = exchange_start(0, 0, [plane_peer(k) for k in range(1, nx * ny)])
    load_in.wait()
    for x in range(ex):
        in_t[:, x * ey * ez:(x + 1) * ey * ez] = in_ref[x].reshape(ey * ez, chan).T
    halo_x()
    halo_y = halo("gy", 1, shifted.at[1, :, 1], shifted.at[1, :, ey + 1],
                  shifted.at[1, :, ey], shifted.at[1, :, 0])

    sums = exchange_sum(0, 0, weight_sums)
    mean_out = sums[0:1] / fan_count
    var_out = sums[1:2] / fan_count - mean_out * mean_out
    inv_std = lax.rsqrt(var_out + var_eps)
    order = [t for c in (1, 0, 2) for t in range(c, taps, 3)]
    own = std_all.at[me["gx"], me["gy"]]
    for u, t in enumerate(order):
        value = (raw_ref[t] - mean_out) * inv_std
        std[u] = value
        own[u] = value.astype(BF16)
    gather_y = []
    for k in range(1, ny):
        copy = remote(own, own, ay_send.at[k - 1], ay_recv.at[k - 1], {"gy": peer("gy", k)})
        copy.start()
        gather_y.append(copy)

    halo_y()
    for x in range(ex + 2):
        plane = shifted[1, x].astype(F32)
        face_out[0, x] = plane[:, 0, :].astype(BF16)
        face_out[1, x] = plane[:, ez - 1, :].astype(BF16)
    halo_z = halo("gz", 2, face_out.at[0], face_in.at[1], face_out.at[1], face_in.at[0])

    def view(t, start, planes):
        a, b, c = t // 9, (t // 3) % 3, t % 3
        block = shifted[2 - c, pl.ds(start + 2 - a, planes), 2 - b:2 - b + ey]
        return block.reshape(planes * ey * ez, chan)

    chunk = taps // 3

    def filter_chunk(n):
        for u in range(n * chunk, (n + 1) * chunk, 2):
            group = list(range(u, min(u + 2, (n + 1) * chunk)))
            views = [view(order[v], 0, ex) for v in group]
            right = jnp.concatenate(views, axis=1) if len(views) > 1 else views[0]
            product = jnp.dot(in_t[...], right, preferred_element_type=F32)
            for j, v in enumerate(group):
                for gx in range(nx):
                    for gy in range(ny):
                        low = (gx * ny + gy) * rows
                        part[gx, gy, v] = product[low:low + rows, j * chan:(j + 1) * chan]
        copies = []
        span = pl.ds(n * chunk, chunk)
        for k in range(1, nx):
            index = n * (nx - 1) + k - 1
            copy = remote(part.at[peer("gx", k), :, span], recv_x.at[k - 1, :, span],
                          x_send.at[index], x_recv.at[index], {"gx": peer("gx", k)})
            copy.start()
            copies.append(copy)
        return copies

    def rows_chunk(n, copies):
        wait_all(copies)
        span = pl.ds(n * chunk, chunk)
        for gy in range(ny):
            total = part[me["gx"], gy, span]
            for k in range(1, nx):
                total = total + recv_x[k - 1, gy, span]
            send_y[gy, span] = total.astype(BF16)
        sent = []
        for k in range(1, ny):
            index = n * (ny - 1) + k - 1
            copy = remote(send_y.at[peer("gy", k), span], recv_y.at[k - 1, span],
                          y_send.at[index], y_recv.at[index], {"gy": peer("gy", k)})
            copy.start()
            sent.append(copy)
        return sent

    depth_index = lax.broadcasted_iota(jnp.int32, (ey + 2, ez, chan), 1)

    def shift(slot, side, amount, edge):
        for x in range(ex + 2):
            plane = shifted[1, x].astype(F32)
            outer = face_in[side, x].astype(F32)[:, None, :]
            shifted[slot, x] = jnp.where(depth_index == edge, outer, pltpu.roll(plane, amount, 1)).astype(BF16)

    copies_0 = filter_chunk(0)
    halo_z()
    shift(2, 1, ez - 1, ez - 1)
    copies_1 = filter_chunk(1)
    reduce_y = rows_chunk(0, copies_0)
    shift(0, 0, 1, 0)
    copies_2 = filter_chunk(2)
    reduce_y += rows_chunk(1, copies_1)
    wait_all(gather_y)
    gather_x = []
    for k in range(1, nx):
        copy = remote(std_all.at[me["gx"]], std_all.at[me["gx"]], ax_send.at[k - 1], ax_recv.at[k - 1],
                      {"gx": peer("gx", k)})
        copy.start()
        gather_x.append(copy)
    reduce_y += rows_chunk(2, copies_2)

    wait_all(gather_x)
    for u in range(taps):
        w_cat[:, u * chan:(u + 1) * chan] = std_all[:, :, u].reshape(nx * ny * rows, chan)
    step = 2 if ex % 2 == 0 else 1

    def dx_step(n, carry):
        start = n * step
        left = jnp.concatenate([view(t, start, step) for t in order], axis=1)
        product = lax.dot_general(left, w_cat[...], (((1,), (1,)), ((), ())), preferred_element_type=F32)
        dx_ref[pl.ds(start, step)] = product.astype(BF16).reshape(step, ey, ez, chan)
        return carry

    half = ex // step // 2
    lax.fori_loop(0, half, dx_step, 0)

    wait_all(reduce_y)
    total = send_y[me["gy"]].astype(F32)
    for k in range(1, ny):
        total = total + recv_y[k - 1].astype(F32)
    send_z[0:taps] = total.astype(BF16)
    reduce_z = []
    for k in range(1, nz):
        copy = remote(send_z.at[pl.ds(peer("gz", k) * piece, piece)], recv_z.at[k - 1],
                      z_send.at[k - 1], z_recv.at[k - 1], {"gz": peer("gz", k)})
        copy.start()
        reduce_z.append(copy)

    lax.fori_loop(half, ex // step, dx_step, 0)

    wait_all(reduce_z)
    mine = pl.ds(me["gz"] * piece, piece)
    grad = send_z[mine].astype(F32)
    for k in range(1, nz):
        grad = grad + recv_z[k - 1].astype(F32)
    full[mine] = grad
    stats[1] = jnp.concatenate(
        [per_output(grad), per_output(grad * std[mine]), per_output(grad * grad), jnp.zeros((5, chan), F32)], axis=0
    )
    depth_peers = [{"gz": peer("gz", k)} for k in range(1, nz)]
    sums_z = exchange_start(1, plane_peers, depth_peers)
    gather_z = []
    for k in range(1, nz):
        copy = remote(full.at[mine], full.at[mine], g_send.at[k - 1], g_recv.at[k - 1], {"gz": peer("gz", k)})
        copy.start()
        gather_z.append(copy)
    stats[2] = exchange_sum(1, plane_peers, sums_z)
    sums_xy = exchange_start(2, plane_peers + nz - 1, [plane_peer(k) for k in range(1, nx * ny)])
    wait_all(gather_z)
    sums = exchange_sum(2, plane_peers + nz - 1, sums_xy)
    sum_grad, sum_cross, sum_square = sums[0:1], sums[1:2], sums[2:3]
    mean_grad = sum_grad / fan_count
    mean_cross = sum_cross / fan_count
    spread = sum_square - 2.0 * mean_grad * sum_grad - 2.0 * mean_cross * sum_cross
    spread = (
        spread
        + fan_count * mean_grad * mean_grad
        + fan_count * mean_cross * mean_cross * var_out / (var_out + var_eps)
    )
    square_sum = jnp.sum(inv_std * inv_std * spread, axis=1, keepdims=True)
    scale = jnp.minimum(1.0, clip_norm * lax.rsqrt(square_sum + norm_eps))
    factor = inv_std * scale
    for u, t in enumerate(order):
        wg_ref[t] = factor * (full[u] - mean_grad - std[u] * mean_cross)


def on_device(dims, raw_weight, inputs, cotangent):
    nx, ny, nz = dims
    rows, taps, chan = raw_weight.shape
    ex, ey, ez = inputs.shape[:3]
    padded_taps = -(-taps // nz) * nz
    piece = padded_taps // nz
    stat_slots = 2 * (nx * ny - 1) + nz - 1
    dma = pltpu.SemaphoreType.DMA

    def pair(n):
        return [dma((max(n, 1),)), dma((max(n, 1),))]

    scratch = [
        pltpu.VMEM((taps, rows, chan), F32),
        pltpu.VMEM(inputs.shape, BF16),
        pltpu.VMEM((3, ex + 2, ey + 2, ez, chan), BF16),
        pltpu.VMEM((2, ex + 2, ey + 2, chan), BF16),
        pltpu.VMEM((2, ex + 2, ey + 2, chan), BF16),
        pltpu.VMEM((chan, ex * ey * ez), BF16),
        pltpu.VMEM((nx, ny, taps, rows, chan), F32),
        pltpu.VMEM((nx - 1, ny, taps, rows, chan), F32),
        pltpu.VMEM((ny, taps, rows, chan), BF16),
        pltpu.VMEM((ny - 1, taps, rows, chan), BF16),
        pltpu.VMEM((padded_taps, rows, chan), BF16),
        pltpu.VMEM((nz - 1, piece, rows, chan), BF16),
        pltpu.VMEM((padded_taps, rows, chan), F32),
        pltpu.VMEM((padded_taps, rows, chan), F32),
        pltpu.VMEM((nx, ny, taps, rows, chan), BF16),
        pltpu.VMEM((chan, taps * chan), BF16),
        pltpu.VMEM((3, 8, chan), F32),
        pltpu.VMEM((stat_slots, 8, chan), F32),
        dma((3,)), *pair(6), *pair(3 * (nx - 1)), *pair(3 * (ny - 1)), *pair(nz - 1), *pair(nz - 1),
        *pair(ny - 1), *pair(nx - 1), *pair(stat_slots),
    ]
    vmem = pl.BlockSpec(memory_space=pltpu.VMEM)
    anywhere = pl.BlockSpec(memory_space=pl.ANY)
    input_grad, weight_grad = pl.pallas_call(
        functools.partial(kernel, dims),
        out_shape=(
            jax.ShapeDtypeStruct(cotangent.shape, BF16),
            jax.ShapeDtypeStruct((taps, rows, chan), F32),
        ),
        in_specs=[anywhere] * 3,
        out_specs=(vmem, vmem),
        scratch_shapes=scratch,
        compiler_params=pltpu.CompilerParams(
            collective_id=0, has_side_effects=True, vmem_limit_bytes=60 * 1024 * 1024
        ),
    )(jnp.transpose(raw_weight, (1, 0, 2)), inputs, cotangent)
    return input_grad, jnp.transpose(weight_grad, (1, 0, 2))


def solution(mesh):
    dims = tuple(mesh.shape[axis] for axis in AXES)
    in_specs = (P(("gx", "gy"), None, None), P("gx", "gy", "gz", None), P("gx", "gy", "gz", None))
    out_specs = (P("gx", "gy", "gz", None), P(("gx", "gy"), None, None))
    return jax.shard_map(
        functools.partial(on_device, dims), mesh=mesh, in_specs=in_specs, out_specs=out_specs, check_vma=False
    )
```

```python
import functools

import jax
import jax.numpy as jnp
from jax import lax
from jax.experimental import pallas as pl
from jax.experimental.pallas import tpu as pltpu
from jax.sharding import PartitionSpec as P

var_eps = 1e-05
norm_eps = 1e-06
clip_norm = 600.0
F32 = jnp.float32
BF16 = jnp.bfloat16
MESH = pl.DeviceIdType.MESH
AXES = ("gx", "gy", "gz")


def z_groups(taps, nz):
    chunk = taps // 3
    sizes = [-(-2 * chunk // nz), -(-chunk // nz)]
    return [(0, 0, 2 * chunk, sizes[0]), (sizes[0] * nz, 2 * chunk, chunk, sizes[1])]


def kernel(dims, raw_hbm, in_hbm, cot_hbm, dx_ref, wg_ref, *scratch):
    (raw_ref, in_ref, shifted, face_out, face_in, in_t, part, recv_x, send_y, recv_y, send_z, recv_z, full, std,
     std_all, w_cat, stats, stats_in, load_sem, halo_send, halo_recv, x_send, x_recv, y_send, y_recv,
     z_send, z_recv, g_send, g_recv, ay_send, ay_recv, ax_send, ax_recv, st_send, st_recv) = scratch
    count = dict(zip(AXES, dims))
    nx, ny, nz = dims
    plane_peers = nx * ny - 1
    me = {axis: lax.axis_index(axis) for axis in AXES}
    taps, rows, chan = raw_ref.shape
    ex, ey, ez = in_ref.shape[:3]
    chunk = taps // 3
    groups = z_groups(taps, nz)
    fan_count = float(rows * nx * ny * taps)

    def peer(axis, k):
        return lax.rem(me[axis] + k, count[axis])

    def plane_peer(k):
        flat = lax.rem(me["gx"] * ny + me["gy"] + k, nx * ny)
        return {"gx": lax.div(flat, ny), "gy": lax.rem(flat, ny)}

    def remote(src, dst, send_sem, recv_sem, where):
        return pltpu.make_async_remote_copy(
            src_ref=src, dst_ref=dst, send_sem=send_sem, recv_sem=recv_sem,
            device_id=where, device_id_type=MESH,
        )

    def wait_all(copies):
        for copy in copies:
            copy.wait()

    body = pl.ds(1, ey)
    load_raw = pltpu.make_async_copy(raw_hbm, raw_ref, load_sem.at[0])
    load_cot = pltpu.make_async_copy(cot_hbm, shifted.at[1, pl.ds(1, ex), body], load_sem.at[1])
    load_in = pltpu.make_async_copy(in_hbm, in_ref, load_sem.at[2])
    load_raw.start()
    load_cot.start()
    load_in.start()

    barrier = pltpu.get_barrier_semaphore()
    for k in range(1, nx * ny):
        pl.semaphore_signal(barrier, inc=1, device_id=plane_peer(k), device_id_type=MESH)
    for k in range(1, nz):
        pl.semaphore_signal(barrier, inc=1, device_id={"gz": peer("gz", k)}, device_id_type=MESH)

    def exchange_start(slot, base, peers):
        copies = []
        for k, where in enumerate(peers):
            copy = remote(stats.at[slot], stats_in.at[base + k], st_send.at[base + k], st_recv.at[base + k], where)
            copy.start()
            copies.append(copy)
        return copies

    def exchange_sum(slot, base, copies):
        wait_all(copies)
        total = stats[slot]
        for k in range(len(copies)):
            total = total + stats_in[base + k]
        return total

    zero_plane = jnp.zeros((ey + 2, ez, chan), BF16)
    zero_col = jnp.zeros((ex + 2, ez, chan), BF16)
    zero_face = jnp.zeros((ex + 2, ey + 2, chan), BF16)

    @pl.when(me["gx"] == 0)
    def _():
        shifted[1, 0] = zero_plane

    @pl.when(me["gx"] == nx - 1)
    def _():
        shifted[1, ex + 1] = zero_plane

    @pl.when(me["gy"] == 0)
    def _():
        shifted[1, :, 0] = zero_col

    @pl.when(me["gy"] == ny - 1)
    def _():
        shifted[1, :, ey + 1] = zero_col

    @pl.when(me["gz"] == 0)
    def _():
        face_in[0] = zero_face

    @pl.when(me["gz"] == nz - 1)
    def _():
        face_in[1] = zero_face

    for t in [b + v for b, first, many, size in groups for v in range(many, size * nz)]:
        send_z[t] = jnp.zeros((rows, chan), BF16)
        std[t] = jnp.zeros((rows, chan), F32)

    load_raw.wait()

    def per_output(value):
        return jnp.sum(jnp.sum(value, axis=0), axis=0, keepdims=True)

    raw = raw_ref[...]
    stats[0] = jnp.concatenate([per_output(raw), per_output(raw * raw), jnp.zeros((6, chan), F32)], axis=0)
    load_cot.wait()
    pl.semaphore_wait(barrier, plane_peers + nz - 1)

    def halo(axis, number, low_src, high_dst, high_src, low_dst):
        lower, upper = lax.max(me[axis] - 1, 0), lax.min(me[axis] + 1, count[axis] - 1)
        down = remote(low_src, high_dst, halo_send.at[2 * number], halo_recv.at[2 * number], {axis: lower})
        up = remote(high_src, low_dst, halo_send.at[2 * number + 1], halo_recv.at[2 * number + 1], {axis: upper})

        @pl.when(me[axis] > 0)
        def _():
            down.start()

        @pl.when(me[axis] < count[axis] - 1)
        def _():
            up.start()

        def finish():
            @pl.when(me[axis] > 0)
            def _():
                down.wait_send()
                up.wait_recv()

            @pl.when(me[axis] < count[axis] - 1)
            def _():
                up.wait_send()
                down.wait_recv()

        return finish

    def inside(dx, dy):
        gx, gy = me["gx"] + dx, me["gy"] + dy
        within = jnp.logical_and(gx >= 0, gx < nx)
        return jnp.logical_and(within, jnp.logical_and(gy >= 0, gy < ny))

    plane_halo = []
    for dx, dy in [(0, -1), (0, 1), (-1, 0), (1, 0), (-1, -1), (-1, 1), (1, -1), (1, 1)]:
        src_x = {-1: 1, 0: pl.ds(1, ex), 1: ex}[dx]
        dst_x = {-1: ex + 1, 0: pl.ds(1, ex), 1: 0}[dx]
        src_y = {-1: 1, 0: body, 1: ey}[dy]
        dst_y = {-1: ey + 1, 0: body, 1: 0}[dy]
        where = {
            "gx": lax.min(lax.max(me["gx"] + dx, 0), nx - 1),
            "gy": lax.min(lax.max(me["gy"] + dy, 0), ny - 1),
        }
        number = 2 + len(plane_halo)
        copy = remote(shifted.at[1, src_x, src_y], shifted.at[1, dst_x, dst_y],
                      halo_send.at[number], halo_recv.at[number], where)
        pl.when(inside(dx, dy))(copy.start)
        plane_halo.append((dx, dy, copy))
    weight_sums = exchange_start(0, 0, [plane_peer(k) for k in range(1, nx * ny)])
    load_in.wait()
    for x in range(ex):
        in_t[:, x * ey * ez:(x + 1) * ey * ez] = in_ref[x].reshape(ey * ez, chan).T
    sums = exchange_sum(0, 0, weight_sums)
    mean_out = sums[0:1] / fan_count
    var_out = sums[1:2] / fan_count - mean_out * mean_out
    inv_std = lax.rsqrt(var_out + var_eps)
    order = [t for c in (1, 0, 2) for t in range(c, taps, 3)]
    slots = [b + v for b, first, many, size in groups for v in range(many)]
    own = std_all.at[me["gx"], me["gy"]]
    for u, t in enumerate(order):
        value = (raw_ref[t] - mean_out) * inv_std
        std[slots[u]] = value
        own[u] = value.astype(BF16)
    gather_y = []
    for k in range(1, ny):
        copy = remote(own, own, ay_send.at[k - 1], ay_recv.at[k - 1], {"gy": peer("gy", k)})
        copy.start()
        gather_y.append(copy)

    for dx, dy, copy in plane_halo:
        pl.when(inside(dx, dy))(copy.wait_send)
        pl.when(inside(-dx, -dy))(copy.wait_recv)
    for x in range(ex + 2):
        plane = shifted[1, x].astype(F32)
        face_out[0, x] = plane[:, 0, :].astype(BF16)
        face_out[1, x] = plane[:, ez - 1, :].astype(BF16)
    halo_z = halo("gz", 0, face_out.at[0], face_in.at[1], face_out.at[1], face_in.at[0])

    def view(t, start, planes):
        a, b, c = t // 9, (t // 3) % 3, t % 3
        block = shifted[2 - c, pl.ds(start + 2 - a, planes), 2 - b:2 - b + ey]
        return block.reshape(planes * ey * ez, chan)

    def filter_chunk(n):
        for u in range(n * chunk, (n + 1) * chunk, 2):
            group = list(range(u, min(u + 2, (n + 1) * chunk)))
            views = [view(order[v], 0, ex) for v in group]
            right = jnp.concatenate(views, axis=1) if len(views) > 1 else views[0]
            product = jnp.dot(in_t[...], right, preferred_element_type=F32)
            for j, v in enumerate(group):
                for gx in range(nx):
                    for gy in range(ny):
                        low = (gx * ny + gy) * rows
                        part[gx, gy, v] = product[low:low + rows, j * chan:(j + 1) * chan]
        copies = []
        span = pl.ds(n * chunk, chunk)
        for k in range(1, nx):
            index = n * (nx - 1) + k - 1
            copy = remote(part.at[peer("gx", k), :, span], recv_x.at[k - 1, :, span],
                          x_send.at[index], x_recv.at[index], {"gx": peer("gx", k)})
            copy.start()
            copies.append(copy)
        return copies

    def rows_chunk(n, copies):
        wait_all(copies)
        span = pl.ds(n * chunk, chunk)
        for gy in range(ny):
            total = part[me["gx"], gy, span]
            for k in range(1, nx):
                total = total + recv_x[k - 1, gy, span]
            send_y[gy, span] = total.astype(BF16)
        sent = []
        for k in range(1, ny):
            index = n * (ny - 1) + k - 1
            copy = remote(send_y.at[peer("gy", k), span], recv_y.at[k - 1, span],
                          y_send.at[index], y_recv.at[index], {"gy": peer("gy", k)})
            copy.start()
            sent.append(copy)
        return sent

    depth_index = lax.broadcasted_iota(jnp.int32, (ey + 2, ez, chan), 1)

    def shift(slot, side, amount, edge):
        for x in range(ex + 2):
            plane = shifted[1, x].astype(F32)
            outer = face_in[side, x].astype(F32)[:, None, :]
            shifted[slot, x] = jnp.where(depth_index == edge, outer, pltpu.roll(plane, amount, 1)).astype(BF16)

    copies_0 = filter_chunk(0)
    halo_z()
    shift(2, 1, ez - 1, ez - 1)
    copies_1 = filter_chunk(1)
    reduce_y = [rows_chunk(0, copies_0)]
    shift(0, 0, 1, 0)
    copies_2 = filter_chunk(2)
    reduce_y.append(rows_chunk(1, copies_1))
    wait_all(gather_y)
    gather_x = []
    for k in range(1, nx):
        copy = remote(std_all.at[me["gx"]], std_all.at[me["gx"]], ax_send.at[k - 1], ax_recv.at[k - 1],
                      {"gx": peer("gx", k)})
        copy.start()
        gather_x.append(copy)
    reduce_y.append(rows_chunk(2, copies_2))

    wait_all(gather_x)
    for u in range(taps):
        w_cat[:, u * chan:(u + 1) * chan] = std_all[:, :, u].reshape(nx * ny * rows, chan)
    step = 2 if ex % 2 == 0 else 1

    def dx_step(n, carry):
        start = n * step
        left = jnp.concatenate([view(t, start, step) for t in order], axis=1)
        product = lax.dot_general(left, w_cat[...], (((1,), (1,)), ((), ())), preferred_element_type=F32)
        dx_ref[pl.ds(start, step)] = product.astype(BF16).reshape(step, ey, ez, chan)
        return carry

    steps = ex // step
    marks = [0, steps // 4, steps * 3 // 4, steps]

    def depth_start(g):
        base, first, many, size = groups[g]
        span = pl.ds(first, many)
        total = send_y[me["gy"], span].astype(F32)
        for k in range(1, ny):
            total = total + recv_y[k - 1, span].astype(F32)
        send_z[base:base + many] = total.astype(BF16)
        copies = []
        for k in range(1, nz):
            index = g * (nz - 1) + k - 1
            copy = remote(send_z.at[pl.ds(base + peer("gz", k) * size, size)],
                          recv_z.at[k - 1, pl.ds(base // nz, size)],
                          z_send.at[index], z_recv.at[index], {"gz": peer("gz", k)})
            copy.start()
            copies.append(copy)
        return copies

    def depth_sum(g, copies):
        wait_all(copies)
        base, first, many, size = groups[g]
        mine = pl.ds(base + me["gz"] * size, size)
        grad = send_z[mine].astype(F32)
        for k in range(1, nz):
            grad = grad + recv_z[k - 1, pl.ds(base // nz, size)].astype(F32)
        full[mine] = grad.astype(BF16)
        sums = [per_output(grad), per_output(grad * std[mine]), per_output(grad * grad)]
        return jnp.concatenate(sums + [jnp.zeros((5, chan), F32)], axis=0)

    def gather_start(g):
        base, first, many, size = groups[g]
        mine = pl.ds(base + me["gz"] * size, size)
        copies = []
        for k in range(1, nz):
            index = g * (nz - 1) + k - 1
            copy = remote(full.at[mine], full.at[mine], g_send.at[index], g_recv.at[index], {"gz": peer("gz", k)})
            copy.start()
            copies.append(copy)
        return copies

    lax.fori_loop(marks[0], marks[1], dx_step, 0)
    wait_all(reduce_y[0] + reduce_y[1])
    reduce_0 = depth_start(0)
    lax.fori_loop(marks[1], marks[2], dx_step, 0)
    wait_all(reduce_y[2])
    reduce_1 = depth_start(1)
    lax.fori_loop(marks[2], marks[3], dx_step, 0)
    first_sums = depth_sum(0, reduce_0)
    gather_z = gather_start(0)
    stats[1] = first_sums + depth_sum(1, reduce_1)
    depth_peers = [{"gz": peer("gz", k)} for k in range(1, nz)]
    sums_z = exchange_start(1, plane_peers, depth_peers)
    gather_z += gather_start(1)
    stats[2] = exchange_sum(1, plane_peers, sums_z)
    sums_xy = exchange_start(2, plane_peers + nz - 1, [plane_peer(k) for k in range(1, nx * ny)])
    wait_all(gather_z)
    sums = exchange_sum(2, plane_peers + nz - 1, sums_xy)
    sum_grad, sum_cross, sum_square = sums[0:1], sums[1:2], sums[2:3]
    mean_grad = sum_grad / fan_count
    mean_cross = sum_cross / fan_count
    spread = sum_square - 2.0 * mean_grad * sum_grad - 2.0 * mean_cross * sum_cross
    spread = (
        spread
        + fan_count * mean_grad * mean_grad
        + fan_count * mean_cross * mean_cross * var_out / (var_out + var_eps)
    )
    square_sum = jnp.sum(inv_std * inv_std * spread, axis=1, keepdims=True)
    scale = jnp.minimum(1.0, clip_norm * lax.rsqrt(square_sum + norm_eps))
    factor = inv_std * scale
    for u, t in enumerate(order):
        value = full[slots[u]].astype(F32)
        wg_ref[t] = factor * (value - mean_grad - std[slots[u]] * mean_cross)


def on_device(dims, raw_weight, inputs, cotangent):
    nx, ny, nz = dims
    rows, taps, chan = raw_weight.shape
    ex, ey, ez = inputs.shape[:3]
    groups = z_groups(taps, nz)
    piece = sum(size for base, first, many, size in groups)
    padded_taps = piece * nz
    stat_slots = 2 * (nx * ny - 1) + nz - 1
    dma = pltpu.SemaphoreType.DMA

    def pair(n):
        return [dma((max(n, 1),)), dma((max(n, 1),))]

    scratch = [
        pltpu.VMEM((taps, rows, chan), F32),
        pltpu.VMEM(inputs.shape, BF16),
        pltpu.VMEM((3, ex + 2, ey + 2, ez, chan), BF16),
        pltpu.VMEM((2, ex + 2, ey + 2, chan), BF16),
        pltpu.VMEM((2, ex + 2, ey + 2, chan), BF16),
        pltpu.VMEM((chan, ex * ey * ez), BF16),
        pltpu.VMEM((nx, ny, taps, rows, chan), F32),
        pltpu.VMEM((nx - 1, ny, taps, rows, chan), F32),
        pltpu.VMEM((ny, taps, rows, chan), BF16),
        pltpu.VMEM((ny - 1, taps, rows, chan), BF16),
        pltpu.VMEM((padded_taps, rows, chan), BF16),
        pltpu.VMEM((nz - 1, piece, rows, chan), BF16),
        pltpu.VMEM((padded_taps, rows, chan), BF16),
        pltpu.VMEM((padded_taps, rows, chan), F32),
        pltpu.VMEM((nx, ny, taps, rows, chan), BF16),
        pltpu.VMEM((chan, taps * chan), BF16),
        pltpu.VMEM((3, 8, chan), F32),
        pltpu.VMEM((stat_slots, 8, chan), F32),
        dma((3,)), *pair(10), *pair(3 * (nx - 1)), *pair(3 * (ny - 1)), *pair(2 * (nz - 1)), *pair(2 * (nz - 1)),
        *pair(ny - 1), *pair(nx - 1), *pair(stat_slots),
    ]
    vmem = pl.BlockSpec(memory_space=pltpu.VMEM)
    anywhere = pl.BlockSpec(memory_space=pl.ANY)
    input_grad, weight_grad = pl.pallas_call(
        functools.partial(kernel, dims),
        out_shape=(
            jax.ShapeDtypeStruct(cotangent.shape, BF16),
            jax.ShapeDtypeStruct((taps, rows, chan), F32),
        ),
        in_specs=[anywhere] * 3,
        out_specs=(vmem, vmem),
        scratch_shapes=scratch,
        compiler_params=pltpu.CompilerParams(
            collective_id=0, has_side_effects=True, vmem_limit_bytes=60 * 1024 * 1024
        ),
    )(jnp.transpose(raw_weight, (1, 0, 2)), inputs, cotangent)
    return input_grad, jnp.transpose(weight_grad, (1, 0, 2))


def solution(mesh):
    dims = tuple(mesh.shape[axis] for axis in AXES)
    in_specs = (P(("gx", "gy"), None, None), P("gx", "gy", "gz", None), P("gx", "gy", "gz", None))
    out_specs = (P("gx", "gy", "gz", None), P(("gx", "gy"), None, None))
    return jax.shard_map(
        functools.partial(on_device, dims), mesh=mesh, in_specs=in_specs, out_specs=out_specs, check_vma=False
    )
```

```python
import functools

import jax
import jax.numpy as jnp
from jax import lax
from jax.experimental import pallas as pl
from jax.experimental.pallas import tpu as pltpu
from jax.sharding import PartitionSpec as P

var_eps = 1e-05
norm_eps = 1e-06
clip_norm = 600.0
F32 = jnp.float32
BF16 = jnp.bfloat16
MESH = pl.DeviceIdType.MESH
AXES = ("gx", "gy", "gz")


def z_groups(taps, nz):
    chunk = taps // 3
    sizes = [-(-2 * chunk // nz), -(-chunk // nz)]
    return [(0, 0, 2 * chunk, sizes[0]), (sizes[0] * nz, 2 * chunk, chunk, sizes[1])]


def kernel(dims, raw_hbm, in_hbm, cot_hbm, dx_ref, wg_ref, *scratch):
    (raw_ref, in_ref, shifted, face_out, face_in, in_t, part, recv_x, send_y, recv_y, send_z, recv_z, full, std,
     std_all, w_cat, stats, stats_in, total_in, load_sem, halo_send, halo_recv, x_send, x_recv, y_send, y_recv,
     z_send, z_recv, g_send, g_recv, ay_send, ay_recv, ax_send, ax_recv, st_send, st_recv, t_send, t_recv) = scratch
    count = dict(zip(AXES, dims))
    nx, ny, nz = dims
    plane_peers = nx * ny - 1
    me = {axis: lax.axis_index(axis) for axis in AXES}
    taps, rows, chan = raw_ref.shape
    ex, ey, ez = in_ref.shape[:3]
    chunk = taps // 3
    groups = z_groups(taps, nz)
    fan_count = float(rows * nx * ny * taps)

    def peer(axis, k):
        return lax.rem(me[axis] + k, count[axis])

    def plane_peer(k):
        flat = lax.rem(me["gx"] * ny + me["gy"] + k, nx * ny)
        return {"gx": lax.div(flat, ny), "gy": lax.rem(flat, ny)}

    def remote(src, dst, send_sem, recv_sem, where):
        return pltpu.make_async_remote_copy(
            src_ref=src, dst_ref=dst, send_sem=send_sem, recv_sem=recv_sem,
            device_id=where, device_id_type=MESH,
        )

    def wait_all(copies):
        for copy in copies:
            copy.wait()

    body = pl.ds(1, ey)
    load_raw = pltpu.make_async_copy(raw_hbm, raw_ref, load_sem.at[0])
    load_cot = pltpu.make_async_copy(cot_hbm, shifted.at[1, pl.ds(1, ex), body], load_sem.at[1])
    load_in = pltpu.make_async_copy(in_hbm, in_ref, load_sem.at[2])
    load_raw.start()
    load_cot.start()
    load_in.start()

    barrier = pltpu.get_barrier_semaphore()
    for k in range(1, nx * ny):
        pl.semaphore_signal(barrier, inc=1, device_id=plane_peer(k), device_id_type=MESH)
    for k in range(1, nz):
        pl.semaphore_signal(barrier, inc=1, device_id={"gz": peer("gz", k)}, device_id_type=MESH)

    def exchange_start(slot, base, peers):
        copies = []
        for k, where in enumerate(peers):
            copy = remote(stats.at[slot], stats_in.at[base + k], st_send.at[base + k], st_recv.at[base + k], where)
            copy.start()
            copies.append(copy)
        return copies

    def exchange_sum(slot, base, copies):
        wait_all(copies)
        total = stats[slot]
        for k in range(len(copies)):
            total = total + stats_in[base + k]
        return total

    zero_plane = jnp.zeros((ey + 2, ez, chan), BF16)
    zero_col = jnp.zeros((ex + 2, ez, chan), BF16)
    zero_face = jnp.zeros((ex + 2, ey + 2, chan), BF16)

    @pl.when(me["gx"] == 0)
    def _():
        shifted[1, 0] = zero_plane

    @pl.when(me["gx"] == nx - 1)
    def _():
        shifted[1, ex + 1] = zero_plane

    @pl.when(me["gy"] == 0)
    def _():
        shifted[1, :, 0] = zero_col

    @pl.when(me["gy"] == ny - 1)
    def _():
        shifted[1, :, ey + 1] = zero_col

    @pl.when(me["gz"] == 0)
    def _():
        face_in[0] = zero_face

    @pl.when(me["gz"] == nz - 1)
    def _():
        face_in[1] = zero_face

    for t in [b + v for b, first, many, size in groups for v in range(many, size * nz)]:
        send_z[t] = jnp.zeros((rows, chan), BF16)
        std[t] = jnp.zeros((rows, chan), F32)

    load_raw.wait()

    def per_output(value):
        return jnp.sum(jnp.sum(value, axis=0), axis=0, keepdims=True)

    raw = raw_ref[...]
    stats[0] = jnp.concatenate([per_output(raw), per_output(raw * raw), jnp.zeros((6, chan), F32)], axis=0)
    pl.semaphore_wait(barrier, plane_peers + nz - 1)
    weight_sums = exchange_start(0, 0, [plane_peer(k) for k in range(1, nx * ny)])
    load_cot.wait()

    def halo(axis, number, low_src, high_dst, high_src, low_dst):
        lower, upper = lax.max(me[axis] - 1, 0), lax.min(me[axis] + 1, count[axis] - 1)
        down = remote(low_src, high_dst, halo_send.at[2 * number], halo_recv.at[2 * number], {axis: lower})
        up = remote(high_src, low_dst, halo_send.at[2 * number + 1], halo_recv.at[2 * number + 1], {axis: upper})

        @pl.when(me[axis] > 0)
        def _():
            down.start()

        @pl.when(me[axis] < count[axis] - 1)
        def _():
            up.start()

        def finish():
            @pl.when(me[axis] > 0)
            def _():
                down.wait_send()
                up.wait_recv()

            @pl.when(me[axis] < count[axis] - 1)
            def _():
                up.wait_send()
                down.wait_recv()

        return finish

    def inside(dx, dy):
        gx, gy = me["gx"] + dx, me["gy"] + dy
        within = jnp.logical_and(gx >= 0, gx < nx)
        return jnp.logical_and(within, jnp.logical_and(gy >= 0, gy < ny))

    plane_halo = []
    for dx, dy in [(0, -1), (0, 1), (-1, 0), (1, 0), (-1, -1), (-1, 1), (1, -1), (1, 1)]:
        src_x = {-1: 1, 0: pl.ds(1, ex), 1: ex}[dx]
        dst_x = {-1: ex + 1, 0: pl.ds(1, ex), 1: 0}[dx]
        src_y = {-1: 1, 0: body, 1: ey}[dy]
        dst_y = {-1: ey + 1, 0: body, 1: 0}[dy]
        where = {
            "gx": lax.min(lax.max(me["gx"] + dx, 0), nx - 1),
            "gy": lax.min(lax.max(me["gy"] + dy, 0), ny - 1),
        }
        number = 2 + len(plane_halo)
        copy = remote(shifted.at[1, src_x, src_y], shifted.at[1, dst_x, dst_y],
                      halo_send.at[number], halo_recv.at[number], where)
        pl.when(inside(dx, dy))(copy.start)
        plane_halo.append((dx, dy, copy))
    load_in.wait()
    for x in range(ex):
        in_t[:, x * ey * ez:(x + 1) * ey * ez] = in_ref[x].reshape(ey * ez, chan).T
    for dx, dy, copy in plane_halo:
        pl.when(inside(dx, dy))(copy.wait_send)
        pl.when(inside(-dx, -dy))(copy.wait_recv)
    for x in range(ex + 2):
        plane = shifted[1, x].astype(F32)
        face_out[0, x] = plane[:, 0, :].astype(BF16)
        face_out[1, x] = plane[:, ez - 1, :].astype(BF16)
    halo_z = halo("gz", 0, face_out.at[0], face_in.at[1], face_out.at[1], face_in.at[0])

    sums = exchange_sum(0, 0, weight_sums)
    mean_out = sums[0:1] / fan_count
    var_out = sums[1:2] / fan_count - mean_out * mean_out
    inv_std = lax.rsqrt(var_out + var_eps)
    order = [t for c in (1, 0, 2) for t in range(c, taps, 3)]
    slots = [b + v for b, first, many, size in groups for v in range(many)]
    own = std_all.at[me["gx"], me["gy"]]
    for u, t in enumerate(order):
        value = (raw_ref[t] - mean_out) * inv_std
        std[slots[u]] = value
        own[u] = value.astype(BF16)
    gather_y = []
    for k in range(1, ny):
        copy = remote(own, own, ay_send.at[k - 1], ay_recv.at[k - 1], {"gy": peer("gy", k)})
        copy.start()
        gather_y.append(copy)

    def view(t, start, planes):
        a, b, c = t // 9, (t // 3) % 3, t % 3
        block = shifted[2 - c, pl.ds(start + 2 - a, planes), 2 - b:2 - b + ey]
        return block.reshape(planes * ey * ez, chan)

    def filter_chunk(n):
        for u in range(n * chunk, (n + 1) * chunk, 2):
            group = list(range(u, min(u + 2, (n + 1) * chunk)))
            views = [view(order[v], 0, ex) for v in group]
            right = jnp.concatenate(views, axis=1) if len(views) > 1 else views[0]
            product = jnp.dot(in_t[...], right, preferred_element_type=F32)
            for j, v in enumerate(group):
                for gx in range(nx):
                    for gy in range(ny):
                        low = (gx * ny + gy) * rows
                        part[gx, gy, v] = product[low:low + rows, j * chan:(j + 1) * chan]
        copies = []
        span = pl.ds(n * chunk, chunk)
        for k in range(1, nx):
            index = n * (nx - 1) + k - 1
            copy = remote(part.at[peer("gx", k), :, span], recv_x.at[k - 1, :, span],
                          x_send.at[index], x_recv.at[index], {"gx": peer("gx", k)})
            copy.start()
            copies.append(copy)
        return copies

    def rows_chunk(n, copies):
        wait_all(copies)
        span = pl.ds(n * chunk, chunk)
        for gy in range(ny):
            total = part[me["gx"], gy, span]
            for k in range(1, nx):
                total = total + recv_x[k - 1, gy, span]
            send_y[gy, span] = total.astype(BF16)
        sent = []
        for k in range(1, ny):
            index = n * (ny - 1) + k - 1
            copy = remote(send_y.at[peer("gy", k), span], recv_y.at[k - 1, span],
                          y_send.at[index], y_recv.at[index], {"gy": peer("gy", k)})
            copy.start()
            sent.append(copy)
        return sent

    depth_index = lax.broadcasted_iota(jnp.int32, (ey + 2, ez, chan), 1)

    def shift(slot, side, amount, edge):
        for x in range(ex + 2):
            plane = shifted[1, x].astype(F32)
            outer = face_in[side, x].astype(F32)[:, None, :]
            shifted[slot, x] = jnp.where(depth_index == edge, outer, pltpu.roll(plane, amount, 1)).astype(BF16)

    copies_0 = filter_chunk(0)
    halo_z()
    shift(2, 1, ez - 1, ez - 1)
    copies_1 = filter_chunk(1)
    reduce_y = [rows_chunk(0, copies_0)]
    shift(0, 0, 1, 0)
    copies_2 = filter_chunk(2)
    reduce_y.append(rows_chunk(1, copies_1))
    reduce_y.append(rows_chunk(2, copies_2))
    wait_all(gather_y)
    gather_x = []
    for k in range(1, nx):
        copy = remote(std_all.at[me["gx"]], std_all.at[me["gx"]], ax_send.at[k - 1], ax_recv.at[k - 1],
                      {"gx": peer("gx", k)})
        copy.start()
        gather_x.append(copy)

    step = 2 if ex % 2 == 0 else 1

    def dx_step(n, carry):
        start = n * step
        left = jnp.concatenate([view(t, start, step) for t in order], axis=1)
        product = lax.dot_general(left, w_cat[...], (((1,), (1,)), ((), ())), preferred_element_type=F32)
        dx_ref[pl.ds(start, step)] = product.astype(BF16).reshape(step, ey, ez, chan)
        return carry

    steps = ex // step
    half = steps // 2

    def depth_start(g):
        base, first, many, size = groups[g]
        span = pl.ds(first, many)
        total = send_y[me["gy"], span].astype(F32)
        for k in range(1, ny):
            total = total + recv_y[k - 1, span].astype(F32)
        send_z[base:base + many] = total.astype(BF16)
        copies = []
        for k in range(1, nz):
            index = g * (nz - 1) + k - 1
            copy = remote(send_z.at[pl.ds(base + peer("gz", k) * size, size)],
                          recv_z.at[k - 1, pl.ds(base // nz, size)],
                          z_send.at[index], z_recv.at[index], {"gz": peer("gz", k)})
            copy.start()
            copies.append(copy)
        return copies

    def depth_sum(g, copies):
        wait_all(copies)
        base, first, many, size = groups[g]
        mine = pl.ds(base + me["gz"] * size, size)
        grad = send_z[mine].astype(F32)
        for k in range(1, nz):
            grad = grad + recv_z[k - 1, pl.ds(base // nz, size)].astype(F32)
        full[mine] = grad.astype(BF16)
        sums = [per_output(grad), per_output(grad * std[mine]), per_output(grad * grad)]
        return jnp.concatenate(sums + [jnp.zeros((5, chan), F32)], axis=0)

    def gather_start(g):
        base, first, many, size = groups[g]
        mine = pl.ds(base + me["gz"] * size, size)
        copies = []
        for k in range(1, nz):
            index = g * (nz - 1) + k - 1
            copy = remote(full.at[mine], full.at[mine], g_send.at[index], g_recv.at[index], {"gz": peer("gz", k)})
            copy.start()
            copies.append(copy)
        return copies

    wait_all(reduce_y[0] + reduce_y[1])
    reduce_0 = depth_start(0)
    wait_all(gather_x)
    for u in range(taps):
        w_cat[:, u * chan:(u + 1) * chan] = std_all[:, :, u].reshape(nx * ny * rows, chan)
    lax.fori_loop(0, half, dx_step, 0)
    wait_all(reduce_y[2])
    reduce_1 = depth_start(1)
    lax.fori_loop(half, steps, dx_step, 0)
    first_sums = depth_sum(0, reduce_0)
    gather_z = gather_start(0)
    stats[1] = first_sums + depth_sum(1, reduce_1)
    flat = (me["gx"] * ny + me["gy"]) * nz + me["gz"]
    total_in[flat] = stats[1]
    final_sums = []
    for k in range(1, nx * ny * nz):
        other = lax.rem(flat + k, nx * ny * nz)
        where = {
            "gx": lax.div(other, ny * nz),
            "gy": lax.rem(lax.div(other, nz), ny),
            "gz": lax.rem(other, nz),
        }
        copy = remote(stats.at[1], total_in.at[flat], t_send.at[k - 1], t_recv.at[k - 1], where)
        copy.start()
        final_sums.append(copy)
    gather_z += gather_start(1)
    wait_all(final_sums)
    sums = total_in[0]
    for k in range(1, nx * ny * nz):
        sums = sums + total_in[k]
    wait_all(gather_z)
    sum_grad, sum_cross, sum_square = sums[0:1], sums[1:2], sums[2:3]
    mean_grad = sum_grad / fan_count
    mean_cross = sum_cross / fan_count
    spread = sum_square - 2.0 * mean_grad * sum_grad - 2.0 * mean_cross * sum_cross
    spread = (
        spread
        + fan_count * mean_grad * mean_grad
        + fan_count * mean_cross * mean_cross * var_out / (var_out + var_eps)
    )
    square_sum = jnp.sum(inv_std * inv_std * spread, axis=1, keepdims=True)
    scale = jnp.minimum(1.0, clip_norm * lax.rsqrt(square_sum + norm_eps))
    factor = inv_std * scale
    for u, t in enumerate(order):
        value = full[slots[u]].astype(F32)
        wg_ref[t] = factor * (value - mean_grad - std[slots[u]] * mean_cross)


def on_device(dims, raw_weight, inputs, cotangent):
    nx, ny, nz = dims
    rows, taps, chan = raw_weight.shape
    ex, ey, ez = inputs.shape[:3]
    groups = z_groups(taps, nz)
    piece = sum(size for base, first, many, size in groups)
    padded_taps = piece * nz
    stat_slots = nx * ny - 1
    dma = pltpu.SemaphoreType.DMA

    def pair(n):
        return [dma((max(n, 1),)), dma((max(n, 1),))]

    scratch = [
        pltpu.VMEM((taps, rows, chan), F32),
        pltpu.VMEM(inputs.shape, BF16),
        pltpu.VMEM((3, ex + 2, ey + 2, ez, chan), BF16),
        pltpu.VMEM((2, ex + 2, ey + 2, chan), BF16),
        pltpu.VMEM((2, ex + 2, ey + 2, chan), BF16),
        pltpu.VMEM((chan, ex * ey * ez), BF16),
        pltpu.VMEM((nx, ny, taps, rows, chan), F32),
        pltpu.VMEM((nx - 1, ny, taps, rows, chan), F32),
        pltpu.VMEM((ny, taps, rows, chan), BF16),
        pltpu.VMEM((ny - 1, taps, rows, chan), BF16),
        pltpu.VMEM((padded_taps, rows, chan), BF16),
        pltpu.VMEM((nz - 1, piece, rows, chan), BF16),
        pltpu.VMEM((padded_taps, rows, chan), BF16),
        pltpu.VMEM((padded_taps, rows, chan), F32),
        pltpu.VMEM((nx, ny, taps, rows, chan), BF16),
        pltpu.VMEM((chan, taps * chan), BF16),
        pltpu.VMEM((2, 8, chan), F32),
        pltpu.VMEM((stat_slots, 8, chan), F32),
        pltpu.VMEM((nx * ny * nz, 8, chan), F32),
        dma((3,)), *pair(10), *pair(3 * (nx - 1)), *pair(3 * (ny - 1)), *pair(2 * (nz - 1)), *pair(2 * (nz - 1)),
        *pair(ny - 1), *pair(nx - 1), *pair(stat_slots), *pair(nx * ny * nz - 1),
    ]
    vmem = pl.BlockSpec(memory_space=pltpu.VMEM)
    anywhere = pl.BlockSpec(memory_space=pl.ANY)
    input_grad, weight_grad = pl.pallas_call(
        functools.partial(kernel, dims),
        out_shape=(
            jax.ShapeDtypeStruct(cotangent.shape, BF16),
            jax.ShapeDtypeStruct((taps, rows, chan), F32),
        ),
        in_specs=[anywhere] * 3,
        out_specs=(vmem, vmem),
        scratch_shapes=scratch,
        compiler_params=pltpu.CompilerParams(
            collective_id=0, has_side_effects=True, vmem_limit_bytes=60 * 1024 * 1024
        ),
    )(jnp.transpose(raw_weight, (1, 0, 2)), inputs, cotangent)
    return input_grad, jnp.transpose(weight_grad, (1, 0, 2))


def solution(mesh):
    dims = tuple(mesh.shape[axis] for axis in AXES)
    in_specs = (P(("gx", "gy"), None, None), P("gx", "gy", "gz", None), P("gx", "gy", "gz", None))
    out_specs = (P("gx", "gy", "gz", None), P(("gx", "gy"), None, None))
    return jax.shard_map(
        functools.partial(on_device, dims), mesh=mesh, in_specs=in_specs, out_specs=out_specs, check_vma=False
    )
```

```python
import functools

import jax
import jax.numpy as jnp
from jax import lax
from jax.experimental import pallas as pl
from jax.experimental.pallas import tpu as pltpu
from jax.sharding import PartitionSpec as P

var_eps = 1e-05
norm_eps = 1e-06
clip_norm = 600.0
F32 = jnp.float32
BF16 = jnp.bfloat16
MESH = pl.DeviceIdType.MESH
AXES = ("gx", "gy", "gz")


def z_groups(taps, nz):
    chunk = taps // 3
    sizes = [-(-2 * chunk // nz), -(-chunk // nz)]
    return [(0, 0, 2 * chunk, sizes[0]), (sizes[0] * nz, 2 * chunk, chunk, sizes[1])]


def kernel(dims, raw_hbm, in_hbm, cot_hbm, dx_ref, wg_ref, *scratch):
    (raw_ref, in_ref, shifted, face_out, face_in, in_t, part, recv_x, send_y, recv_y, send_z, recv_z, full, std,
     std_all, w_cat, stats, stats_in, total_in, load_sem, halo_send, halo_recv, x_send, x_recv, y_send, y_recv,
     z_send, z_recv, g_send, g_recv, ay_send, ay_recv, ax_send, ax_recv, st_send, st_recv, t_send, t_recv) = scratch
    count = dict(zip(AXES, dims))
    nx, ny, nz = dims
    plane_peers = nx * ny - 1
    me = {axis: lax.axis_index(axis) for axis in AXES}
    taps, rows, chan = raw_ref.shape
    ex, ey, ez = in_ref.shape[:3]
    chunk = taps // 3
    groups = z_groups(taps, nz)
    fan_count = float(rows * nx * ny * taps)

    def peer(axis, k):
        return lax.rem(me[axis] + k, count[axis])

    def plane_peer(k):
        flat = lax.rem(me["gx"] * ny + me["gy"] + k, nx * ny)
        return {"gx": lax.div(flat, ny), "gy": lax.rem(flat, ny)}

    def remote(src, dst, send_sem, recv_sem, where):
        return pltpu.make_async_remote_copy(
            src_ref=src, dst_ref=dst, send_sem=send_sem, recv_sem=recv_sem,
            device_id=where, device_id_type=MESH,
        )

    def wait_all(copies):
        for copy in copies:
            copy.wait()

    body = pl.ds(1, ey)
    load_raw = pltpu.make_async_copy(raw_hbm, raw_ref, load_sem.at[0])
    load_cot = pltpu.make_async_copy(cot_hbm, shifted.at[1, pl.ds(1, ex), body], load_sem.at[1])
    load_in = pltpu.make_async_copy(in_hbm, in_ref, load_sem.at[2])
    load_raw.start()
    load_cot.start()
    load_in.start()

    barrier = pltpu.get_barrier_semaphore()
    for k in range(1, nx * ny):
        pl.semaphore_signal(barrier, inc=1, device_id=plane_peer(k), device_id_type=MESH)
    for k in range(1, nz):
        pl.semaphore_signal(barrier, inc=1, device_id={"gz": peer("gz", k)}, device_id_type=MESH)

    def exchange_start(slot, base, peers):
        copies = []
        for k, where in enumerate(peers):
            copy = remote(stats.at[slot], stats_in.at[base + k], st_send.at[base + k], st_recv.at[base + k], where)
            copy.start()
            copies.append(copy)
        return copies

    def exchange_sum(slot, base, copies):
        wait_all(copies)
        total = stats[slot]
        for k in range(len(copies)):
            total = total + stats_in[base + k]
        return total

    zero_plane = jnp.zeros((ey + 2, ez, chan), BF16)
    zero_col = jnp.zeros((ex + 2, ez, chan), BF16)
    zero_face = jnp.zeros((ex + 2, ey + 2, chan), BF16)

    @pl.when(me["gx"] == 0)
    def _():
        shifted[1, 0] = zero_plane

    @pl.when(me["gx"] == nx - 1)
    def _():
        shifted[1, ex + 1] = zero_plane

    @pl.when(me["gy"] == 0)
    def _():
        shifted[1, :, 0] = zero_col

    @pl.when(me["gy"] == ny - 1)
    def _():
        shifted[1, :, ey + 1] = zero_col

    @pl.when(me["gz"] == 0)
    def _():
        face_in[0] = zero_face

    @pl.when(me["gz"] == nz - 1)
    def _():
        face_in[1] = zero_face

    for t in [b + v for b, first, many, size in groups for v in range(many, size * nz)]:
        send_z[t] = jnp.zeros((rows, chan), BF16)
        std[t] = jnp.zeros((rows, chan), F32)

    load_raw.wait()

    def per_output(value):
        return jnp.sum(jnp.sum(value, axis=0), axis=0, keepdims=True)

    raw = raw_ref[...]
    stats[0] = jnp.concatenate([per_output(raw), per_output(raw * raw), jnp.zeros((6, chan), F32)], axis=0)
    pl.semaphore_wait(barrier, plane_peers + nz - 1)
    weight_sums = exchange_start(0, 0, [plane_peer(k) for k in range(1, nx * ny)])
    load_cot.wait()

    def halo(axis, number, low_src, high_dst, high_src, low_dst):
        lower, upper = lax.max(me[axis] - 1, 0), lax.min(me[axis] + 1, count[axis] - 1)
        down = remote(low_src, high_dst, halo_send.at[2 * number], halo_recv.at[2 * number], {axis: lower})
        up = remote(high_src, low_dst, halo_send.at[2 * number + 1], halo_recv.at[2 * number + 1], {axis: upper})

        @pl.when(me[axis] > 0)
        def _():
            down.start()

        @pl.when(me[axis] < count[axis] - 1)
        def _():
            up.start()

        def finish():
            @pl.when(me[axis] > 0)
            def _():
                down.wait_send()
                up.wait_recv()

            @pl.when(me[axis] < count[axis] - 1)
            def _():
                up.wait_send()
                down.wait_recv()

        return finish

    def inside(dx, dy):
        gx, gy = me["gx"] + dx, me["gy"] + dy
        within = jnp.logical_and(gx >= 0, gx < nx)
        return jnp.logical_and(within, jnp.logical_and(gy >= 0, gy < ny))

    plane_halo = []
    for dx, dy in [(0, -1), (0, 1), (-1, 0), (1, 0), (-1, -1), (-1, 1), (1, -1), (1, 1)]:
        src_x = {-1: 1, 0: pl.ds(1, ex), 1: ex}[dx]
        dst_x = {-1: ex + 1, 0: pl.ds(1, ex), 1: 0}[dx]
        src_y = {-1: 1, 0: body, 1: ey}[dy]
        dst_y = {-1: ey + 1, 0: body, 1: 0}[dy]
        where = {
            "gx": lax.min(lax.max(me["gx"] + dx, 0), nx - 1),
            "gy": lax.min(lax.max(me["gy"] + dy, 0), ny - 1),
        }
        number = 2 + len(plane_halo)
        copy = remote(shifted.at[1, src_x, src_y], shifted.at[1, dst_x, dst_y],
                      halo_send.at[number], halo_recv.at[number], where)
        pl.when(inside(dx, dy))(copy.start)
        plane_halo.append((dx, dy, copy))
    load_in.wait()
    for x in range(ex):
        in_t[:, x * ey * ez:(x + 1) * ey * ez] = in_ref[x].reshape(ey * ez, chan).T
    for dx, dy, copy in plane_halo:
        pl.when(inside(dx, dy))(copy.wait_send)
        pl.when(inside(-dx, -dy))(copy.wait_recv)
    for x in range(ex + 2):
        plane = shifted[1, x].astype(F32)
        face_out[0, x] = plane[:, 0, :].astype(BF16)
        face_out[1, x] = plane[:, ez - 1, :].astype(BF16)
    halo_z = halo("gz", 0, face_out.at[0], face_in.at[1], face_out.at[1], face_in.at[0])

    sums = exchange_sum(0, 0, weight_sums)
    mean_out = sums[0:1] / fan_count
    var_out = sums[1:2] / fan_count - mean_out * mean_out
    inv_std = lax.rsqrt(var_out + var_eps)
    order = [t for c in (1, 0, 2) for t in range(c, taps, 3)]
    slots = [b + v for b, first, many, size in groups for v in range(many)]
    own = std_all.at[me["gx"], me["gy"]]
    for u, t in enumerate(order):
        value = (raw_ref[t] - mean_out) * inv_std
        std[slots[u]] = value
        own[u] = value.astype(BF16)
    gather_y = []
    for k in range(1, ny):
        copy = remote(own, own, ay_send.at[k - 1], ay_recv.at[k - 1], {"gy": peer("gy", k)})
        copy.start()
        gather_y.append(copy)

    def view(t, start, planes):
        a, b, c = t // 9, (t // 3) % 3, t % 3
        block = shifted[2 - c, pl.ds(start + 2 - a, planes), 2 - b:2 - b + ey]
        return block.reshape(planes * ey * ez, chan)

    def filter_chunk(n):
        for u in range(n * chunk, (n + 1) * chunk, 2):
            group = list(range(u, min(u + 2, (n + 1) * chunk)))
            views = [view(order[v], 0, ex) for v in group]
            right = jnp.concatenate(views, axis=1) if len(views) > 1 else views[0]
            product = jnp.dot(in_t[...], right, preferred_element_type=F32)
            for j, v in enumerate(group):
                for gx in range(nx):
                    for gy in range(ny):
                        low = (gx * ny + gy) * rows
                        part[gx, gy, v] = product[low:low + rows, j * chan:(j + 1) * chan]
        copies = []
        span = pl.ds(n * chunk, chunk)
        for k in range(1, nx):
            index = n * (nx - 1) + k - 1
            copy = remote(part.at[peer("gx", k), :, span], recv_x.at[k - 1, :, span],
                          x_send.at[index], x_recv.at[index], {"gx": peer("gx", k)})
            copy.start()
            copies.append(copy)
        return copies

    def rows_chunk(n, copies):
        wait_all(copies)
        span = pl.ds(n * chunk, chunk)
        for gy in range(ny):
            total = part[me["gx"], gy, span]
            for k in range(1, nx):
                total = total + recv_x[k - 1, gy, span]
            send_y[gy, span] = total.astype(BF16)
        sent = []
        for k in range(1, ny):
            index = n * (ny - 1) + k - 1
            copy = remote(send_y.at[peer("gy", k), span], recv_y.at[k - 1, span],
                          y_send.at[index], y_recv.at[index], {"gy": peer("gy", k)})
            copy.start()
            sent.append(copy)
        return sent

    depth_index = lax.broadcasted_iota(jnp.int32, (ey + 2, ez, chan), 1)

    def shift(slot, side, amount, edge):
        for x in range(ex + 2):
            plane = shifted[1, x].astype(F32)
            outer = face_in[side, x].astype(F32)[:, None, :]
            shifted[slot, x] = jnp.where(depth_index == edge, outer, pltpu.roll(plane, amount, 1)).astype(BF16)

    copies_0 = filter_chunk(0)
    halo_z()
    shift(2, 1, ez - 1, ez - 1)
    copies_1 = filter_chunk(1)
    reduce_y = [rows_chunk(0, copies_0)]
    shift(0, 0, 1, 0)
    copies_2 = filter_chunk(2)
    reduce_y.append(rows_chunk(1, copies_1))
    reduce_y.append(rows_chunk(2, copies_2))
    wait_all(gather_y)
    gather_x = []
    for k in range(1, nx):
        copy = remote(std_all.at[me["gx"]], std_all.at[me["gx"]], ax_send.at[k - 1], ax_recv.at[k - 1],
                      {"gx": peer("gx", k)})
        copy.start()
        gather_x.append(copy)

    step = 2 if ex % 2 == 0 else 1

    def dx_step(n, carry):
        start = n * step
        left = jnp.concatenate([view(t, start, step) for t in order], axis=1)
        product = lax.dot_general(left, w_cat[...], (((1,), (1,)), ((), ())), preferred_element_type=F32)
        dx_ref[pl.ds(start, step)] = product.astype(BF16).reshape(step, ey, ez, chan)
        return carry

    steps = ex // step
    half = steps // 2

    def depth_start(g):
        base, first, many, size = groups[g]
        span = pl.ds(first, many)
        total = send_y[me["gy"], span].astype(F32)
        for k in range(1, ny):
            total = total + recv_y[k - 1, span].astype(F32)
        send_z[base:base + many] = total.astype(BF16)
        copies = []
        for k in range(1, nz):
            index = g * (nz - 1) + k - 1
            copy = remote(send_z.at[pl.ds(base + peer("gz", k) * size, size)],
                          recv_z.at[k - 1, pl.ds(base // nz, size)],
                          z_send.at[index], z_recv.at[index], {"gz": peer("gz", k)})
            copy.start()
            copies.append(copy)
        return copies

    def depth_sum(g, copies):
        wait_all(copies)
        base, first, many, size = groups[g]
        mine = pl.ds(base + me["gz"] * size, size)
        grad = send_z[mine].astype(F32)
        for k in range(1, nz):
            grad = grad + recv_z[k - 1, pl.ds(base // nz, size)].astype(F32)
        full[mine] = grad.astype(BF16)
        sums = [per_output(grad), per_output(grad * std[mine]), per_output(grad * grad)]
        return jnp.concatenate(sums + [jnp.zeros((5, chan), F32)], axis=0)

    def gather_start(g):
        base, first, many, size = groups[g]
        mine = pl.ds(base + me["gz"] * size, size)
        copies = []
        for k in range(1, nz):
            index = g * (nz - 1) + k - 1
            copy = remote(full.at[mine], full.at[mine], g_send.at[index], g_recv.at[index], {"gz": peer("gz", k)})
            copy.start()
            copies.append(copy)
        return copies

    wait_all(gather_x)
    for u in range(taps):
        w_cat[:, u * chan:(u + 1) * chan] = std_all[:, :, u].reshape(nx * ny * rows, chan)
    lax.fori_loop(0, half, dx_step, 0)
    wait_all(reduce_y[0] + reduce_y[1])
    reduce_0 = depth_start(0)
    wait_all(reduce_y[2])
    reduce_1 = depth_start(1)
    lax.fori_loop(half, steps, dx_step, 0)
    first_sums = depth_sum(0, reduce_0)
    gather_z = gather_start(0)
    stats[1] = first_sums + depth_sum(1, reduce_1)
    flat = (me["gx"] * ny + me["gy"]) * nz + me["gz"]
    total_in[flat] = stats[1]
    final_sums = []
    for k in range(1, nx * ny * nz):
        other = lax.rem(flat + k, nx * ny * nz)
        where = {
            "gx": lax.div(other, ny * nz),
            "gy": lax.rem(lax.div(other, nz), ny),
            "gz": lax.rem(other, nz),
        }
        copy = remote(stats.at[1], total_in.at[flat], t_send.at[k - 1], t_recv.at[k - 1], where)
        copy.start()
        final_sums.append(copy)
    gather_z += gather_start(1)
    wait_all(final_sums)
    sums = total_in[0]
    for k in range(1, nx * ny * nz):
        sums = sums + total_in[k]
    wait_all(gather_z)
    sum_grad, sum_cross, sum_square = sums[0:1], sums[1:2], sums[2:3]
    mean_grad = sum_grad / fan_count
    mean_cross = sum_cross / fan_count
    spread = sum_square - 2.0 * mean_grad * sum_grad - 2.0 * mean_cross * sum_cross
    spread = (
        spread
        + fan_count * mean_grad * mean_grad
        + fan_count * mean_cross * mean_cross * var_out / (var_out + var_eps)
    )
    square_sum = jnp.sum(inv_std * inv_std * spread, axis=1, keepdims=True)
    scale = jnp.minimum(1.0, clip_norm * lax.rsqrt(square_sum + norm_eps))
    factor = inv_std * scale
    for u, t in enumerate(order):
        value = full[slots[u]].astype(F32)
        wg_ref[t] = factor * (value - mean_grad - std[slots[u]] * mean_cross)


def on_device(dims, raw_weight, inputs, cotangent):
    nx, ny, nz = dims
    rows, taps, chan = raw_weight.shape
    ex, ey, ez = inputs.shape[:3]
    groups = z_groups(taps, nz)
    piece = sum(size for base, first, many, size in groups)
    padded_taps = piece * nz
    stat_slots = nx * ny - 1
    dma = pltpu.SemaphoreType.DMA

    def pair(n):
        return [dma((max(n, 1),)), dma((max(n, 1),))]

    scratch = [
        pltpu.VMEM((taps, rows, chan), F32),
        pltpu.VMEM(inputs.shape, BF16),
        pltpu.VMEM((3, ex + 2, ey + 2, ez, chan), BF16),
        pltpu.VMEM((2, ex + 2, ey + 2, chan), BF16),
        pltpu.VMEM((2, ex + 2, ey + 2, chan), BF16),
        pltpu.VMEM((chan, ex * ey * ez), BF16),
        pltpu.VMEM((nx, ny, taps, rows, chan), F32),
        pltpu.VMEM((nx - 1, ny, taps, rows, chan), F32),
        pltpu.VMEM((ny, taps, rows, chan), BF16),
        pltpu.VMEM((ny - 1, taps, rows, chan), BF16),
        pltpu.VMEM((padded_taps, rows, chan), BF16),
        pltpu.VMEM((nz - 1, piece, rows, chan), BF16),
        pltpu.VMEM((padded_taps, rows, chan), BF16),
        pltpu.VMEM((padded_taps, rows, chan), F32),
        pltpu.VMEM((nx, ny, taps, rows, chan), BF16),
        pltpu.VMEM((chan, taps * chan), BF16),
        pltpu.VMEM((2, 8, chan), F32),
        pltpu.VMEM((stat_slots, 8, chan), F32),
        pltpu.VMEM((nx * ny * nz, 8, chan), F32),
        dma((3,)), *pair(10), *pair(3 * (nx - 1)), *pair(3 * (ny - 1)), *pair(2 * (nz - 1)), *pair(2 * (nz - 1)),
        *pair(ny - 1), *pair(nx - 1), *pair(stat_slots), *pair(nx * ny * nz - 1),
    ]
    vmem = pl.BlockSpec(memory_space=pltpu.VMEM)
    anywhere = pl.BlockSpec(memory_space=pl.ANY)
    input_grad, weight_grad = pl.pallas_call(
        functools.partial(kernel, dims),
        out_shape=(
            jax.ShapeDtypeStruct(cotangent.shape, BF16),
            jax.ShapeDtypeStruct((taps, rows, chan), F32),
        ),
        in_specs=[anywhere] * 3,
        out_specs=(vmem, vmem),
        scratch_shapes=scratch,
        compiler_params=pltpu.CompilerParams(
            collective_id=0, has_side_effects=True, vmem_limit_bytes=60 * 1024 * 1024
        ),
    )(jnp.transpose(raw_weight, (1, 0, 2)), inputs, cotangent)
    return input_grad, jnp.transpose(weight_grad, (1, 0, 2))


def solution(mesh):
    dims = tuple(mesh.shape[axis] for axis in AXES)
    in_specs = (P(("gx", "gy"), None, None), P("gx", "gy", "gz", None), P("gx", "gy", "gz", None))
    out_specs = (P("gx", "gy", "gz", None), P(("gx", "gy"), None, None))
    return jax.shard_map(
        functools.partial(on_device, dims), mesh=mesh, in_specs=in_specs, out_specs=out_specs, check_vma=False
    )
```
